32 devices in a mesh: expert: 16 (over z, y, x), dp: 2 (over core).
Axes of the slice: x: 2, y: 2, z: 4, core: 2. Of those that a mesh axis runs over, the one named last changes fastest.
Arguments:
- patches: bfloat16 [512, 196, 1024], P(('dp', 'expert')), parts along dimension 0, may hold values from -6 to 6
- visible: int32 [512, 49], P(('dp', 'expert')), parts along dimension 0, may hold values from 0 to 195, as said below
- routes: int32 [25088, 1], P(('dp', 'expert')), parts along dimension 0, may hold values from 0 to 15; in each aligned block of 784 rows (0 to 783, 784 to 1567, ...) at most 74 rows name the same one
- expert_cap: int32 [32], P('dp'), parts along dimension 0, may hold values from 36 to 74
- norm_gain: float32 [1024], replicated, may hold values from 0.5 to 2
- norm_bias: float32 [1024], replicated, may hold values from -6 to 6
- router: float32 [1024, 16], replicated, may hold values from -0.1875 to 0.1875
- w_in: bfloat16 [16, 1024, 4096], P('expert'), may hold values from -0.1875 to 0.1875
- b_in: float32 [16, 4096], P('expert'), may hold values from -6 to 6
- w_out: bfloat16 [16, 4096, 1024], P('expert'), may hold values from -0.09375 to 0.09375
- b_out: float32 [16, 1024], P('expert'), may hold values from -6 to 6
Outputs:
- layer_out: bfloat16 [25088, 1024], P(('dp', 'expert')), parts along dimension 0
The draws below stay inside these ranges and needn't reach their ends.
There are 2 independent parts, one for each index of `dp`. The reference program is written for one: setup_inputs(seed, part) draws one part's arguments, and reference() takes and returns one part's arrays. A program takes and returns all parts, laid end to end along the dimension named above; an argument that names none is the same for every part. Nothing has to cross between parts.
Inputs may be any that keep to these rules, and one draw needn't show every extreme that they name: `visible`: each row holds 49 different patch indices in increasing order. `routes`: among the tokens of one index of expert no expert is named more than 74 times.
All inputs are finite; a program needn't handle non-finite values.
Results may differ from the reference program's by a relative error of at most 0.005.
Values may be sent and summed in bfloat16 or wider, within the bound.
A program may use at most 128 MiB of HBM per device.

```python
import math
import jax
import jax.numpy as jnp
import numpy as np
from jax import lax

D = 1024
FF = 4096
PATCHES = 196
KEEP = 49
EXPERTS = 16
IMAGES = 256
TOK_DEV = 784
TOKENS = 12544
CAP = 74
N_EXPERT = 16


def draw_visible(key, part):
    keys = jax.random.split(jax.random.fold_in(key, 7), IMAGES)

    def one_image(k):
        return jnp.sort(jax.random.permutation(k, PATCHES)[:KEEP])
    return jax.vmap(one_image)(keys).astype(jnp.int32)


def with_ends(result, key, smallest, top_value):
    shape = result.shape
    index_at = [jax.random.randint(jax.random.fold_in(key, axis), (), 0, shape[axis]) for axis in range(len(shape))]
    result = result.at[tuple(index_at)].set(smallest)
    longest = shape.index(max(shape))
    index_at[longest] = (index_at[longest] + 1) % shape[longest]
    return result.at[tuple(index_at)].set(top_value)


def block_levels(own_key, shape, cuts, least, high):
    gain, own = 1.0, jax.random.fold_in(own_key, 6)
    for dim, blocks in cuts:
        draws = jnp.exp(jax.random.uniform(jax.random.fold_in(own, dim), (blocks,), jnp.float32, least / len(cuts), high / len(cuts)))
        gain = gain * jnp.repeat(draws, shape[dim] // blocks).reshape([-1 if axis == dim else 1 for axis in range(len(shape))])
    return gain


def assign_block(own_key, own, number, rows, number_of, top, reach, lean):
    order = jax.random.permutation(own_key, number_of)
    heavy_load, common = load_shares(number_of, rows * top, reach, lean, True), load_shares(number_of, rows * top, reach, lean, False)
    places = jnp.arange(number_of)

    def named(tallies, turn):
        used = int((tallies > 0).sum())
        fixed = max(1, used // 4)
        shifted = fixed + (places - fixed + turn * (used - fixed)) % max(1, number_of - fixed)
        return jnp.zeros((number_of,), jnp.int32).at[order[jnp.where(places < fixed, places, shifted)]].set(jnp.asarray(tallies, jnp.int32))

    tallies = jnp.where(number % 4 == 0, named(heavy_load, number // 4), named(common, number - number // 4 - 1))
    mixed = jax.random.permutation(jax.random.fold_in(own, 3), number_of)
    source_of, taker = mixed[0:number_of // 2 * 2:2], mixed[1:number_of // 2 * 2:2]
    slack = jnp.minimum(tallies[source_of] - 1, reach - tallies[taker]) // 2
    slack = jnp.where((source_of == order[0]) | (taker == order[0]) | (tallies[taker] == 0), 0, jnp.maximum(slack, 0))
    shifted = jax.random.randint(jax.random.fold_in(own, 4), (number_of // 2,), 0, 1 << 20) % (slack + 1)
    tallies = tallies.at[source_of].add(-shifted).at[taker].add(shifted)
    labels = jnp.searchsorted(jnp.cumsum(tallies), jnp.arange(rows * top), side="right").astype(jnp.int32)
    table = labels.reshape(top, rows).T
    table = table[jax.random.permutation(jax.random.fold_in(own, 1), rows)]
    turn = jax.random.randint(jax.random.fold_in(own, 2), (rows, 1), 0, top)
    return jnp.take_along_axis(table, (jnp.arange(top)[None, :] + turn) % top, axis=1)


def load_shares(count, total, reach, slope, full):
    loads = [(1 << 20) // math.isqrt(standing ** slope) + 1 for standing in range(1, count + 1)]
    largest = reach if full else min(reach, max(-(-total // count), total * loads[0] // sum(loads)))
    least = 1 if total - largest >= count - 1 else 0
    given, spare = [largest] + [least] * (count - 1), total - largest - least * (count - 1)
    while spare > 0:
        movable = [i for i in range(1, count) if given[i] < largest] or [i for i in range(1, count) if given[i] < reach]
        whole, left = sum([loads[i] for i in movable]), spare
        for i in movable:
            more = min(reach - given[i], max(1, left * loads[i] // whole), spare)
            given[i] = given[i] + more
            spare = spare - more
    return np.array(given)


def gaussian(key, shape, deviation, bound, pieces=(), kind=jnp.bfloat16):
    factor_of = block_levels(key, shape, pieces, -0.22, 0.18) if pieces else 1.0
    result = jax.random.normal(key, shape, jnp.float32) * deviation * factor_of
    return jnp.minimum(jnp.maximum(result, -bound), bound).astype(kind)


def setup_inputs(seed: int = 0, part: int = 0) -> dict:
    splits = jax.random.split(jax.random.key(seed), 12)
    part_keys = jax.random.split(jax.random.fold_in(splits[11], part), 12)
    patches = gaussian(part_keys[0], (IMAGES, PATCHES, D), 1.0, 6.0, ((0, 16),))
    visible = draw_visible(jax.random.fold_in(jax.random.fold_in(splits[11], part), 71), part)
    routes_keys = jax.random.split(jax.random.fold_in(part_keys[2], 1), TOKENS // TOK_DEV)
    routes_turns = jax.random.permutation(jax.random.fold_in(part_keys[2], 3), TOKENS // TOK_DEV)
    routes = jax.vmap(lambda own, number: assign_block(jax.random.fold_in(part_keys[2], 2), own, number, TOK_DEV, EXPERTS, 1, CAP, 2))(routes_keys, routes_turns).reshape((TOKENS, 1))
    expert_cap = with_ends(jax.random.randint(part_keys[3], (EXPERTS,), CAP // 2 - 1, CAP + 1), jax.random.fold_in(part_keys[3], 1), CAP // 2 - 1, CAP).astype(jnp.int32)
    norm_gain = jnp.clip(jnp.exp(jax.random.uniform(splits[4], (D,), jnp.float32, math.log(0.5), math.log(2.0))), 0.5, 2.0)
    norm_bias = gaussian(splits[5], (D,), 1.0, 6.0, (), jnp.float32)
    router = gaussian(splits[6], (D, EXPERTS), D ** -0.5, 0.1875, (), jnp.float32)
    w_in = gaussian(splits[7], (EXPERTS, D, FF), D ** -0.5, 0.1875, ((0, 16),))
    b_in = gaussian(splits[8], (EXPERTS, FF), 1.0, 6.0, ((0, 16),), jnp.float32)
    w_out = gaussian(splits[9], (EXPERTS, FF, D), FF ** -0.5, 0.09375, ((0, 16),))
    b_out = gaussian(splits[10], (EXPERTS, D), 1.0, 6.0, ((0, 16),), jnp.float32)
    return {"patches": patches, "visible": visible, "routes": routes, "expert_cap": expert_cap, "norm_gain": norm_gain, "norm_bias": norm_bias, "router": router, "w_in": w_in, "b_in": b_in, "w_out": w_out, "b_out": b_out}


def reference(patches, visible, routes, expert_cap, norm_gain, norm_bias, router, w_in, b_in, w_out, b_out):
    x = jnp.take_along_axis(patches, visible[:, :, None], axis=1).reshape(TOKENS, D)
    xf = x.astype(jnp.float32)
    mean = lax.optimization_barrier(jnp.mean(xf, axis=1, keepdims=True))
    var = lax.optimization_barrier(jnp.mean((xf - mean) ** 2, axis=1, keepdims=True))
    h = (xf - mean) / jnp.sqrt(var + 1e-06) * norm_gain + norm_bias
    hb = h.astype(jnp.bfloat16)
    chosen = routes[:, 0]
    onehot = (chosen[:, None] == jnp.arange(EXPERTS, dtype=jnp.int32)[None, :]).astype(jnp.int32)
    logits = jnp.dot(h, router, precision=lax.Precision.HIGHEST)
    gate = jax.nn.sigmoid(lax.optimization_barrier(jnp.sum(logits * onehot.astype(jnp.float32), axis=1)))
    blocks = onehot.reshape(N_EXPERT, TOK_DEV, EXPERTS)
    before = (jnp.cumsum(blocks, axis=1) - blocks).reshape(TOKENS, EXPERTS)
    rank = lax.optimization_barrier(jnp.sum(before * onehot, axis=1))
    limit = lax.optimization_barrier(jnp.sum(onehot * expert_cap[None, :], axis=1))
    kept = rank < limit
    source = (jnp.arange(TOKENS, dtype=jnp.int32) // TOK_DEV).astype(jnp.int32)
    rows_each = N_EXPERT * CAP
    dest = jnp.where(kept, chosen * rows_each + source * CAP + rank, EXPERTS * rows_each).astype(jnp.int32)
    buffer = jnp.zeros((EXPERTS * rows_each + 1, D), jnp.bfloat16).at[dest].set(hb)
    buffer = buffer[:-1].reshape(EXPERTS, rows_each, D)

    def expert_step(args):
        rows, first, bias_first, second, bias_second = args
        act = jax.nn.gelu(jnp.dot(rows, first, preferred_element_type=jnp.float32) + bias_first, approximate=True).astype(jnp.bfloat16)
        return (jnp.dot(act, second, preferred_element_type=jnp.float32) + bias_second).astype(jnp.bfloat16)
    results = lax.map(expert_step, (buffer, w_in, b_in, w_out, b_out)).reshape(EXPERTS * rows_each, D)
    picked = results[jnp.minimum(dest, EXPERTS * rows_each - 1)].astype(jnp.float32)
    branch = jnp.where(kept[:, None], gate[:, None] * picked, 0.0)
    return (xf + branch).astype(jnp.bfloat16)
```

```python
import functools

import jax
import jax.numpy as jnp
from jax import lax
from jax.experimental import pallas as pl
from jax.experimental.pallas import tpu as pltpu
from jax.sharding import PartitionSpec as P

F32 = jnp.float32
BF16 = jnp.bfloat16
ANY = pl.BlockSpec(memory_space=pl.ANY)
VMEM = pl.BlockSpec(memory_space=pltpu.VMEM)
VMEM_LIMIT = 60 * 1024 * 1024


def ceil_to(value, unit):
    return -(-value // unit) * unit


def largest_tile(total, limit, unit):
    for tile in range(limit // unit * unit, 0, -unit):
        if total % tile == 0:
            return tile
    return total


def dispatch_kernel(
    stride, patches, wanted, col, col_x, row, row_x, cap_row, cap_col, gain, bias, router,
    x_out, gate_out, dest_out, outgoing, patch_buf, pick, xs, hb, sems,
):
    tokens, width = xs.shape
    experts = router.shape[1]
    slots_all = outgoing.shape[0]

    part = largest_tile(width, 256, 128)

    def load(i):
        at = pl.ds(i * part, part)
        return pltpu.make_async_copy(patches.at[:, at], patch_buf.at[:, at], sems.at[i])

    for i in range(width // part):
        load(i).start()

    chunk = largest_tile(tokens, 128, 16)
    lane = lax.broadcasted_iota(jnp.int32, (chunk, patches.shape[0]), 1)

    @pl.loop(0, tokens // chunk)
    def _(c):
        at = pl.ds(pl.multiple_of(c * chunk, chunk), chunk)
        pick[at, :] = jnp.where(wanted[at, :] == lane, 1.0, 0.0).astype(BF16)

    tri_r = lax.broadcasted_iota(jnp.int32, (tokens, tokens), 0)
    tri_c = lax.broadcasted_iota(jnp.int32, (tokens, tokens), 1)
    hot_row = jnp.where(
        row[...] == lax.broadcasted_iota(jnp.int32, (experts, tokens), 0), 1.0, 0.0
    )
    before_row = jnp.dot(
        hot_row.astype(BF16), jnp.where(tri_r < tri_c, 1.0, 0.0).astype(BF16),
        preferred_element_type=F32,
    )
    rank_row = jnp.sum(before_row * hot_row, axis=0, keepdims=True).astype(jnp.int32)
    limit_row = jnp.sum(
        hot_row * cap_col[...].astype(F32), axis=0, keepdims=True
    ).astype(jnp.int32)
    dest_row = jnp.where(rank_row < limit_row, row_x[...] * stride + rank_row, -1)

    hot_col = jnp.where(
        col[...] == lax.broadcasted_iota(jnp.int32, (tokens, experts), 1), 1.0, 0.0
    )
    before_col = jnp.dot(
        jnp.where(tri_c < tri_r, 1.0, 0.0).astype(BF16), hot_col.astype(BF16),
        preferred_element_type=F32,
    )
    rank_col = jnp.sum(before_col * hot_col, axis=1, keepdims=True).astype(jnp.int32)
    limit_col = jnp.sum(
        hot_col * cap_row[...].astype(F32), axis=1, keepdims=True
    ).astype(jnp.int32)
    dest_out[...] = jnp.where(rank_col < limit_col, col_x[...] * stride + rank_col, -1)

    for i in range(width // part):
        load(i).wait()
        at = pl.ds(i * part, part)
        xs[:, at] = jnp.dot(pick[...], patch_buf[:, at], preferred_element_type=F32)

    for c in range(tokens // chunk):
        at = pl.ds(c * chunk, chunk)
        xf = xs[at, :]
        mean = jnp.mean(xf, axis=1, keepdims=True)
        off = xf - mean
        var = jnp.mean(off * off, axis=1, keepdims=True)
        h = off / jnp.sqrt(var + 1e-06) * gain[...] + bias[...]
        hb[at, :] = h.astype(BF16)
        x_out[at, :] = xf.astype(BF16)
        logits = jnp.dot(h, router[...], precision=lax.Precision.HIGHEST)
        picked_logit = jnp.sum(
            logits * hot_col[c * chunk : (c + 1) * chunk], axis=1, keepdims=True
        )
        gate_out[at, :] = jax.nn.sigmoid(picked_logit)

    step = largest_tile(slots_all, 256, 16)
    slot = lax.broadcasted_iota(jnp.int32, (step, tokens), 0)

    @pl.loop(0, slots_all // step)
    def _(s):
        place = jnp.where(dest_row - s * step == slot, 1.0, 0.0).astype(BF16)
        at = pl.ds(pl.multiple_of(s * step, step), step)
        outgoing[at, :] = jnp.dot(place, hb[...], preferred_element_type=F32).astype(BF16)


def partner_of(me, k):
    bit = 1
    result = me
    while bit <= k:
        if k & bit:
            result = result + bit * (1 - 2 * lax.rem(lax.div(me, bit), 2))
        bit *= 2
    return result


def expert_kernel(
    devices, stride, outgoing, w_in, b_in, w_out, b_out, back, recv, res, act, w1, w2,
    send_sem, recv_sem, bsend_sem, brecv_sem, w_sem,
):
    me = lax.axis_index("expert")
    hidden = w1.shape[1]
    width = w1.shape[0]
    load_1 = pltpu.make_async_copy(w_in.at[0], w1, w_sem.at[0])
    load_2 = pltpu.make_async_copy(w_out.at[0], w2, w_sem.at[1])
    own_in = pltpu.make_async_copy(
        outgoing.at[pl.ds(0, stride)], recv.at[pl.ds(0, stride)], w_sem.at[2]
    )
    own_in.start()
    load_1.start()
    load_2.start()

    barrier = pltpu.get_barrier_semaphore()
    for k in range(1, devices):
        pl.semaphore_signal(
            barrier, inc=1, device_id={"expert": partner_of(me, k)},
            device_id_type=pl.DeviceIdType.MESH,
        )
    pl.semaphore_wait(barrier, devices - 1)

    def forward(k):
        at = pl.ds(k * stride, stride)
        return pltpu.make_async_remote_copy(
            src_ref=outgoing.at[at], dst_ref=recv.at[at], send_sem=send_sem.at[k],
            recv_sem=recv_sem.at[k], device_id={"expert": partner_of(me, k)},
            device_id_type=pl.DeviceIdType.MESH,
        )

    def backward(k):
        at = pl.ds(k * stride, stride)
        return pltpu.make_async_remote_copy(
            src_ref=res.at[at], dst_ref=back.at[at], send_sem=bsend_sem.at[k],
            recv_sem=brecv_sem.at[k], device_id={"expert": partner_of(me, k)},
            device_id_type=pl.DeviceIdType.MESH,
        )

    groups = 4 if devices % 4 == 0 else 1
    size = devices // groups
    send_order = (2, 3, 1, 0) if groups == 4 else (0,)
    work_order = (0, 2, 3, 1) if groups == 4 else (0,)
    for g in send_order:
        for k in range(g * size, (g + 1) * size):
            if k:
                forward(k).start()

    rows = size * stride
    tile_f = largest_tile(hidden, 512, 128)
    tile_d = largest_tile(width, 256, 128)
    own_out = pltpu.make_async_copy(
        res.at[pl.ds(0, stride)], back.at[pl.ds(0, stride)], w_sem.at[3]
    )
    for turn, g in enumerate(work_order):
        for k in range(g * size, (g + 1) * size):
            if k:
                forward(k).wait_recv()
            else:
                own_in.wait()
        base = g * rows
        if turn == 0:
            load_1.wait()

        @pl.loop(0, hidden // tile_f)
        def _(f):
            at = pl.ds(pl.multiple_of(f * tile_f, tile_f), tile_f)
            v = jnp.dot(
                recv[base : base + rows, :], w1[:, at], preferred_element_type=F32
            ) + b_in[:, at]
            act[:, at] = jax.nn.gelu(v, approximate=True).astype(BF16)

        if turn == 0:
            load_2.wait()

        @pl.loop(0, width // tile_d)
        def _(d):
            at = pl.ds(pl.multiple_of(d * tile_d, tile_d), tile_d)
            v = jnp.dot(act[...], w2[:, at], preferred_element_type=F32) + b_out[:, at]
            res[base : base + rows, at] = v.astype(BF16)

        for k in range(g * size, (g + 1) * size):
            if k:
                backward(k).start()
            else:
                own_out.start()

    for k in range(1, devices):
        forward(k).wait_send()
    own_out.wait()
    for k in range(1, devices):
        backward(k).wait()


def combine_kernel(x, gate, dest, back, out):
    slots_all = back.shape[0]
    rows = x.shape[0]
    slot = lax.broadcasted_iota(jnp.int32, (rows, slots_all), 1)
    place = jnp.where(dest[...] == slot, 1.0, 0.0).astype(BF16)
    picked = jnp.dot(place, back[...], preferred_element_type=F32)
    out[...] = (x[...].astype(F32) + gate[...] * picked).astype(BF16)


def per_device(
    patches, visible, routes, expert_cap, norm_gain, norm_bias, router, w_in, b_in, w_out, b_out
):
    images, count, width = patches.shape
    keep = visible.shape[1]
    devices = lax.axis_size("expert")
    experts = expert_cap.shape[0]
    hidden = w_in.shape[2]
    tokens = images * keep
    slots = max(2, (3 * tokens + 2 * experts - 1) // (2 * experts))
    stride = ceil_to(slots, 16)
    total = experts * stride
    me = lax.axis_index("expert").astype(jnp.int32)

    wanted = (visible * images + jnp.arange(images, dtype=jnp.int32)[:, None]).reshape(tokens, 1)
    row = routes.reshape(1, tokens)
    x, gate, dest, outgoing = pl.pallas_call(
        functools.partial(dispatch_kernel, stride),
        out_shape=(
            jax.ShapeDtypeStruct((tokens, width), BF16),
            jax.ShapeDtypeStruct((tokens, 1), F32),
            jax.ShapeDtypeStruct((tokens, 1), jnp.int32),
            jax.ShapeDtypeStruct((total, width), BF16),
        ),
        in_specs=[ANY] + [VMEM] * 10,
        out_specs=(VMEM,) * 4,
        scratch_shapes=[
            pltpu.VMEM((count * images, width), BF16),
            pltpu.VMEM((tokens, count * images), BF16),
            pltpu.VMEM((tokens, width), F32),
            pltpu.VMEM((tokens, width), BF16),
            pltpu.SemaphoreType.DMA((width // largest_tile(width, 256, 128),)),
        ],
        compiler_params=pltpu.CompilerParams(vmem_limit_bytes=VMEM_LIMIT),
        name="dispatch",
    )(
        patches.transpose(1, 0, 2).reshape(count * images, width), wanted, routes, routes ^ me, row, row ^ me,
        expert_cap.reshape(1, experts), expert_cap.reshape(experts, 1),
        norm_gain.reshape(1, width), norm_bias.reshape(1, width), router,
    )

    group = devices // 4 if devices % 4 == 0 else devices
    back = pl.pallas_call(
        functools.partial(expert_kernel, devices, stride),
        out_shape=jax.ShapeDtypeStruct((total, width), BF16),
        in_specs=[ANY, ANY, VMEM, ANY, VMEM],
        out_specs=ANY,
        scratch_shapes=[
            pltpu.VMEM((total, width), BF16),
            pltpu.VMEM((total, width), BF16),
            pltpu.VMEM((group * stride, hidden), BF16),
            pltpu.VMEM((width, hidden), BF16),
            pltpu.VMEM((hidden, width), BF16),
            pltpu.SemaphoreType.DMA((devices,)),
            pltpu.SemaphoreType.DMA((devices,)),
            pltpu.SemaphoreType.DMA((devices,)),
            pltpu.SemaphoreType.DMA((devices,)),
            pltpu.SemaphoreType.DMA((4,)),
        ],
        compiler_params=pltpu.CompilerParams(
            collective_id=0, has_side_effects=True, vmem_limit_bytes=VMEM_LIMIT
        ),
        name="experts",
    )(outgoing, w_in, b_in, w_out, b_out)

    rows = largest_tile(tokens, 256, 16)
    return pl.pallas_call(
        combine_kernel,
        grid=(tokens // rows,),
        out_shape=jax.ShapeDtypeStruct((tokens, width), BF16),
        in_specs=[
            pl.BlockSpec((rows, width), lambda i: (i, 0)),
            pl.BlockSpec((rows, 1), lambda i: (i, 0)),
            pl.BlockSpec((rows, 1), lambda i: (i, 0)),
            pl.BlockSpec((total, width), lambda i: (0, 0)),
        ],
        out_specs=pl.BlockSpec((rows, width), lambda i: (i, 0)),
        compiler_params=pltpu.CompilerParams(vmem_limit_bytes=VMEM_LIMIT),
        name="combine",
    )(x, gate, dest, back)


def solution(mesh):
    return jax.shard_map(
        per_device,
        mesh=mesh,
        in_specs=(
            P(("dp", "expert"), None, None),
            P(("dp", "expert"), None),
            P(("dp", "expert"), None),
            P("dp"),
            P(),
            P(),
            P(),
            P("expert", None, None),
            P("expert", None),
            P("expert", None, None),
            P("expert", None),
        ),
        out_specs=P(("dp", "expert"), None),
        check_vma=False,
    )
```

```python
import functools

import jax
import jax.numpy as jnp
from jax import lax
from jax.experimental import pallas as pl
from jax.experimental.pallas import tpu as pltpu
from jax.sharding import PartitionSpec as P

F32 = jnp.float32
BF16 = jnp.bfloat16
ANY = pl.BlockSpec(memory_space=pl.ANY)
VMEM = pl.BlockSpec(memory_space=pltpu.VMEM)
VMEM_LIMIT = 60 * 1024 * 1024


def ceil_to(value, unit):
    return -(-value // unit) * unit


def largest_tile(total, limit, unit):
    for tile in range(limit // unit * unit, 0, -unit):
        if total % tile == 0:
            return tile
    return total


def dispatch_kernel(
    stride, patches, wanted, row, cap, gain, bias, router_t,
    x_out, gate_out, dest_out, outgoing, patch_buf, pick, xs, hb, sems,
):
    tokens, width = xs.shape
    experts = router_t.shape[0]
    slots_all = outgoing.shape[0]
    me = lax.axis_index("expert")

    part = largest_tile(width, 256, 128)

    def load(i):
        at = pl.ds(i * part, part)
        return pltpu.make_async_copy(patches.at[:, at], patch_buf.at[:, at], sems.at[i])

    for i in range(width // part):
        load(i).start()

    chunk = largest_tile(tokens, 128, 16)
    lane = lax.broadcasted_iota(jnp.int32, (chunk, patches.shape[0]), 1)

    @pl.loop(0, tokens // chunk)
    def _(c):
        at = pl.ds(pl.multiple_of(c * chunk, chunk), chunk)
        pick[at, :] = jnp.where(wanted[at, :] == lane, 1.0, 0.0).astype(BF16)

    tri_r = lax.broadcasted_iota(jnp.int32, (tokens, tokens), 0)
    tri_c = lax.broadcasted_iota(jnp.int32, (tokens, tokens), 1)
    chosen = row[...]
    hot_row = jnp.where(chosen == lax.broadcasted_iota(jnp.int32, (experts, tokens), 0), 1.0, 0.0)
    before = jnp.dot(
        hot_row.astype(BF16), jnp.where(tri_r < tri_c, 1.0, 0.0).astype(BF16),
        preferred_element_type=F32,
    )
    rank = jnp.sum(before * hot_row, axis=0, keepdims=True).astype(jnp.int32)
    caps = jnp.broadcast_to(cap[...].astype(F32), (8, experts))
    limit = jnp.dot(caps, hot_row, precision=lax.Precision.HIGHEST)[0:1]
    dest_row = jnp.where(rank < limit.astype(jnp.int32), (chosen ^ me) * stride + rank, -1)

    digit = lax.broadcasted_iota(jnp.int32, (8, tokens), 0)
    full = dest_row + 1
    digits = jnp.where(
        digit == 0, full >> 7, jnp.where(digit == 1, full & 127, jnp.where(digit == 2, chosen, 0))
    )
    columns = lax.dot_general(
        jnp.where(tri_r == tri_c, 1.0, 0.0).astype(BF16), digits.astype(F32).astype(BF16),
        (((1,), (1,)), ((), ())), preferred_element_type=F32,
    ).astype(jnp.int32)
    dest_out[...] = columns[:, 0:1] * 128 + columns[:, 1:2] - 1
    hot_col = jnp.where(
        columns[:, 2:3] == lax.broadcasted_iota(jnp.int32, (tokens, experts), 1), 1.0, 0.0
    )

    for i in range(width // part):
        load(i).wait()
        at = pl.ds(i * part, part)
        xs[:, at] = jnp.dot(pick[...], patch_buf[:, at], preferred_element_type=F32)

    for c in range(tokens // chunk):
        at = pl.ds(c * chunk, chunk)
        xf = xs[at, :]
        mean = jnp.mean(xf, axis=1, keepdims=True)
        off = xf - mean
        var = jnp.mean(off * off, axis=1, keepdims=True)
        h = off / jnp.sqrt(var + 1e-06) * gain[...] + bias[...]
        hb[at, :] = h.astype(BF16)
        x_out[at, :] = xf.astype(BF16)
        logits = lax.dot_general(
            h, router_t[...], (((1,), (1,)), ((), ())), precision=lax.Precision.HIGHEST,
            preferred_element_type=F32,
        )
        picked_logit = jnp.sum(
            logits * hot_col[c * chunk : (c + 1) * chunk], axis=1, keepdims=True
        )
        gate_out[at, :] = jax.nn.sigmoid(picked_logit)

    step = largest_tile(slots_all, 256, 16)
    slot = lax.broadcasted_iota(jnp.int32, (step, tokens), 0)

    @pl.loop(0, slots_all // step)
    def _(s):
        place = jnp.where(dest_row - s * step == slot, 1.0, 0.0).astype(BF16)
        at = pl.ds(pl.multiple_of(s * step, step), step)
        outgoing[at, :] = jnp.dot(place, hb[...], preferred_element_type=F32).astype(BF16)


def partner_of(me, k):
    bit = 1
    result = me
    while bit <= k:
        if k & bit:
            result = result + bit * (1 - 2 * lax.rem(lax.div(me, bit), 2))
        bit *= 2
    return result


def expert_kernel(
    devices, stride, slots, outgoing, w_in, b_in, w_out, b_out, back, recv, res, act, w1, w2,
    send_sem, recv_sem, bsend_sem, brecv_sem, w_sem,
):
    me = lax.axis_index("expert")
    hidden = w1.shape[1]
    width = w1.shape[0]
    load_1 = pltpu.make_async_copy(w_in.at[0], w1, w_sem.at[0])
    load_2 = pltpu.make_async_copy(w_out.at[0], w2, w_sem.at[1])
    if slots < stride:
        recv[...] = jnp.zeros_like(recv)
    own_in = pltpu.make_async_copy(
        outgoing.at[pl.ds(0, stride)], recv.at[pl.ds(0, stride)], w_sem.at[2]
    )
    own_in.start()
    load_1.start()
    load_2.start()

    barrier = pltpu.get_barrier_semaphore()
    for k in range(1, devices):
        pl.semaphore_signal(
            barrier, inc=1, device_id={"expert": partner_of(me, k)},
            device_id_type=pl.DeviceIdType.MESH,
        )
    pl.semaphore_wait(barrier, devices - 1)

    def forward(k):
        at = pl.ds(k * stride, slots)
        return pltpu.make_async_remote_copy(
            src_ref=outgoing.at[at], dst_ref=recv.at[at], send_sem=send_sem.at[k],
            recv_sem=recv_sem.at[k], device_id={"expert": partner_of(me, k)},
            device_id_type=pl.DeviceIdType.MESH,
        )

    def backward(k):
        at = pl.ds(k * stride, slots)
        return pltpu.make_async_remote_copy(
            src_ref=res.at[at], dst_ref=back.at[at], send_sem=bsend_sem.at[k],
            recv_sem=brecv_sem.at[k], device_id={"expert": partner_of(me, k)},
            device_id_type=pl.DeviceIdType.MESH,
        )

    groups = 4 if devices % 4 == 0 else 1
    size = devices // groups
    send_order = (2, 3, 1, 0) if groups == 4 else (0,)
    work_order = (0, 2, 1, 3) if groups == 4 else (0,)
    for g in send_order:
        for k in range(g * size, (g + 1) * size):
            if k:
                forward(k).start()

    rows = size * stride
    tile_f = largest_tile(hidden, 512, 128)
    tile_d = largest_tile(width, 256, 128)
    own_out = pltpu.make_async_copy(
        res.at[pl.ds(0, stride)], back.at[pl.ds(0, stride)], w_sem.at[3]
    )
    for turn, g in enumerate(work_order):
        for k in range(g * size, (g + 1) * size):
            if k:
                forward(k).wait_recv()
            else:
                own_in.wait()
        base = g * rows
        if turn == 0:
            load_1.wait()

        @pl.loop(0, hidden // tile_f)
        def _(f):
            at = pl.ds(pl.multiple_of(f * tile_f, tile_f), tile_f)
            v = jnp.dot(
                recv[base : base + rows, :], w1[:, at], preferred_element_type=F32
            ) + b_in[:, at]
            act[:, at] = jax.nn.gelu(v, approximate=True).astype(BF16)

        if turn == 0:
            load_2.wait()

        @pl.loop(0, width // tile_d)
        def _(d):
            at = pl.ds(pl.multiple_of(d * tile_d, tile_d), tile_d)
            v = jnp.dot(act[...], w2[:, at], preferred_element_type=F32) + b_out[:, at]
            res[base : base + rows, at] = v.astype(BF16)

        for k in range(g * size, (g + 1) * size):
            if k:
                backward(k).start()
            else:
                own_out.start()

    for k in range(1, devices):
        forward(k).wait_send()
    own_out.wait()
    for k in range(1, devices):
        backward(k).wait()


def combine_kernel(stride, slots, x, gate, dest, back, out, place):
    slots_all = back.shape[0]
    rows = x.shape[0]
    chunk = largest_tile(rows, 128, 16)

    @pl.when(pl.program_id(0) == 0)
    def _():
        slot = lax.broadcasted_iota(jnp.int32, (chunk, slots_all), 1)

        @pl.loop(0, rows // chunk)
        def _(c):
            at = pl.ds(pl.multiple_of(c * chunk, chunk), chunk)
            place[at, :] = jnp.where(dest[at, :] == slot, 1.0, 0.0).astype(BF16)

    used = lax.rem(lax.broadcasted_iota(jnp.int32, back.shape, 0), stride) < slots
    result = jnp.where(used, back[...], jnp.zeros((), BF16))
    picked = jnp.dot(place[...], result, preferred_element_type=F32)
    out[...] = (x[...].astype(F32) + gate[...] * picked).astype(BF16)


def per_device(
    patches, visible, routes, expert_cap, norm_gain, norm_bias, router, w_in, b_in, w_out, b_out
):
    images, count, width = patches.shape
    keep = visible.shape[1]
    devices = lax.axis_size("expert")
    experts = expert_cap.shape[0]
    hidden = w_in.shape[2]
    tokens = images * keep
    slots = max(2, (3 * tokens + 2 * experts - 1) // (2 * experts))
    stride = ceil_to(slots, 16)
    total = experts * stride

    wanted = (visible * images + jnp.arange(images, dtype=jnp.int32)[:, None]).reshape(tokens, 1)
    row = routes.reshape(1, tokens)
    x, gate, dest, outgoing = pl.pallas_call(
        functools.partial(dispatch_kernel, stride),
        out_shape=(
            jax.ShapeDtypeStruct((tokens, width), BF16),
            jax.ShapeDtypeStruct((tokens, 1), F32),
            jax.ShapeDtypeStruct((tokens, 1), jnp.int32),
            jax.ShapeDtypeStruct((total, width), BF16),
        ),
        in_specs=[ANY] + [VMEM] * 6,
        out_specs=(VMEM,) * 4,
        scratch_shapes=[
            pltpu.VMEM((count * images, width), BF16),
            pltpu.VMEM((tokens, count * images), BF16),
            pltpu.VMEM((tokens, width), F32),
            pltpu.VMEM((tokens, width), BF16),
            pltpu.SemaphoreType.DMA((width // largest_tile(width, 256, 128),)),
        ],
        compiler_params=pltpu.CompilerParams(vmem_limit_bytes=VMEM_LIMIT),
        name="dispatch",
    )(
        patches.transpose(1, 0, 2).reshape(count * images, width), wanted, row,
        expert_cap.reshape(1, experts),
        norm_gain.reshape(1, width), norm_bias.reshape(1, width), router.T,
    )

    sent = ceil_to(slots, 8)
    group = devices // 4 if devices % 4 == 0 else devices
    back = pl.pallas_call(
        functools.partial(expert_kernel, devices, stride, sent),
        out_shape=jax.ShapeDtypeStruct((total, width), BF16),
        in_specs=[ANY, ANY, VMEM, ANY, VMEM],
        out_specs=ANY,
        scratch_shapes=[
            pltpu.VMEM((total, width), BF16),
            pltpu.VMEM((total, width), BF16),
            pltpu.VMEM((group * stride, hidden), BF16),
            pltpu.VMEM((width, hidden), BF16),
            pltpu.VMEM((hidden, width), BF16),
            pltpu.SemaphoreType.DMA((devices,)),
            pltpu.SemaphoreType.DMA((devices,)),
            pltpu.SemaphoreType.DMA((devices,)),
            pltpu.SemaphoreType.DMA((devices,)),
            pltpu.SemaphoreType.DMA((4,)),
        ],
        compiler_params=pltpu.CompilerParams(
            collective_id=0, has_side_effects=True, vmem_limit_bytes=VMEM_LIMIT
        ),
        name="experts",
    )(outgoing, w_in, b_in, w_out, b_out)

    tile = largest_tile(width, 256, 128)
    return pl.pallas_call(
        functools.partial(combine_kernel, stride, slots),
        grid=(width // tile,),
        out_shape=jax.ShapeDtypeStruct((tokens, width), BF16),
        in_specs=[
            pl.BlockSpec((tokens, tile), lambda i: (0, i)),
            pl.BlockSpec((tokens, 1), lambda i: (0, 0)),
            pl.BlockSpec((tokens, 1), lambda i: (0, 0)),
            pl.BlockSpec((total, tile), lambda i: (0, i)),
        ],
        out_specs=pl.BlockSpec((tokens, tile), lambda i: (0, i)),
        scratch_shapes=[pltpu.VMEM((tokens, total), BF16)],
        compiler_params=pltpu.CompilerParams(vmem_limit_bytes=VMEM_LIMIT),
        name="combine",
    )(x, gate, dest, back)


def solution(mesh):
    return jax.shard_map(
        per_device,
        mesh=mesh,
        in_specs=(
            P(("dp", "expert"), None, None),
            P(("dp", "expert"), None),
            P(("dp", "expert"), None),
            P("dp"),
            P(),
            P(),
            P(),
            P("expert", None, None),
            P("expert", None),
            P("expert", None, None),
            P("expert", None),
        ),
        out_specs=P(("dp", "expert"), None),
        check_vma=False,
    )
```
